32 devices in a mesh: dp: 2 (over x), c: 4 (over z), r: 4 (over y, core).
Axes of the slice: x: 2, y: 2, z: 4, core: 2. Of those that a mesh axis runs over, the one named last changes fastest.
Arguments:
- x: bfloat16 [6144, 3584], P(('dp', 'r'), 'c'), parts along dimension 0
- w: bfloat16 [3584, 28672], P('r', 'c')
- dy: bfloat16 [6144, 28672], P(('dp', 'r'), 'c'), parts along dimension 0
Outputs:
- output 1: bfloat16 [6144, 3584], P(('dp', 'r'), 'c'), parts along dimension 0
- output 2: float32 [7168, 28672], P(('dp', 'r'), 'c'), parts along dimension 0
There are 2 independent parts. The reference program is written for one: setup_inputs(seed, part) draws one part's arguments, and reference() takes and returns one part's arrays. A program takes and returns all parts, laid end to end along the dimension named above; an argument that names none is the same for every part.
All inputs are finite; a program needn't handle non-finite values.
Results may differ from the reference program's by a relative error of at most 0.001.
Values are sent between devices in bfloat16 or wider.
A program may use at most 1 GiB of HBM per device.

```python
import jax
import jax.numpy as jnp

T = 3072
H = 3584
F = 14336


def setup_inputs(seed: int = 0, part: int = 0) -> dict:
    base = jax.random.PRNGKey(seed)
    kw, kpart = jax.random.split(base)
    kx, kdy = jax.random.split(jax.random.fold_in(kpart, part))
    n = 2 * F
    x = jax.random.normal(kx, (T, H), jnp.float32)
    w = jax.random.normal(kw, (H, n), jnp.float32) * H ** -0.5
    dy = jax.random.normal(kdy, (T, n), jnp.float32) * (T * n / H) ** -0.25
    return {"x": x.astype(jnp.bfloat16), "w": w.astype(jnp.bfloat16), "dy": dy.astype(jnp.bfloat16)}


def reference(x, w, dy):
    dx = jnp.dot(dy, w.T, preferred_element_type=jnp.float32).astype(jnp.bfloat16)
    dw = jnp.dot(x.T, dy, preferred_element_type=jnp.float32)
    return dx, dw
```

```python
import jax
import jax.numpy as jnp
from jax import lax
from jax.experimental import pallas as pl
from jax.experimental.pallas import tpu as pltpu
from jax.sharding import PartitionSpec as P

N = 4
ANY = pl.BlockSpec(memory_space=pl.ANY)
PIECES = 12
CHUNKS = 2 * PIECES
THIRD = PIECES // 2


def exchange(xt_ref, w_ref, dy_ref, dx_ref, dyg_ref, xg_ref,
             wv, dyv, pv, upv, dnv, ov, xv,
             x_s, xu_s, xd_s, x_r, y_s, y_r, o_s, o_r, f_s, f_r, c_s, cu_r, cd_r, b_s, b_r, ld, aux):
    r = lax.axis_index("r")
    z = lax.axis_index("c")
    r1 = r + 1 - 2 * (r % 2)
    r2 = (r + 2) % N
    r3 = N - 1 - r
    mx = ((r // 2 + z // 2) % 2) * 2 + (r % 2 + z % 2) % 2
    diag = r == z
    has_up = jnp.logical_and(z >= r, z < N - 1)
    has_dn = jnp.logical_and(z <= r, z > 0)
    rows = dy_ref.shape[0]
    p = rows // PIECES
    n = w_ref.shape[1]
    kb = n // 7

    def far(src, dst, s, d, **where):
        return pltpu.make_async_remote_copy(src_ref=src, dst_ref=dst, send_sem=s, recv_sem=d, device_id=where,
                                            device_id_type=pl.DeviceIdType.MESH)

    def piece(q, cnt=1):
        return pl.ds(pl.multiple_of(q * p, p), cnt * p)

    barrier = pltpu.get_barrier_semaphore()
    for peer in (r1, r2, r3):
        pl.semaphore_signal(barrier, inc=1, device_id={"r": peer}, device_id_type=pl.DeviceIdType.MESH)

    @pl.when(z > 0)
    def _():
        pl.semaphore_signal(barrier, inc=1, device_id={"c": z - 1}, device_id_type=pl.DeviceIdType.MESH)

    @pl.when(z < N - 1)
    def _():
        pl.semaphore_signal(barrier, inc=1, device_id={"c": z + 1}, device_id_type=pl.DeviceIdType.MESH)

    pl.semaphore_wait(barrier, jnp.where(jnp.logical_or(z == 0, z == N - 1), 4, 5))

    def x_send():
        return far(xt_ref, xg_ref.at[mx], x_s.at[0], x_r.at[mx], r=z)

    def x_up(src, m):
        return far(src, xg_ref.at[m], xu_s.at[m], x_r.at[m], c=z + 1)

    def x_dn(src, m):
        return far(src, xg_ref.at[m], xd_s.at[m], x_r.at[m], c=z - 1)

    @pl.when(jnp.logical_not(diag))
    def _():
        x_send().start()

    def y_send(q):
        return far(dy_ref.at[piece(q)], dyg_ref.at[1, piece(q)], y_s.at[q], y_r.at[q], r=r2)

    def o_send(q):
        return far(dy_ref.at[piece(2 * q, 2)], dyg_ref.at[0, piece(2 * q, 2)], o_s.at[q], o_r.at[q], r=r1)

    def f_send(q):
        return far(dyg_ref.at[1, piece(q)], dyg_ref.at[2, piece(q)], f_s.at[q], f_r.at[q], r=r1)

    @pl.loop(0, PIECES)
    def _(q):
        y_send(q).start()

    w_load = pltpu.make_async_copy(w_ref, wv, aux.at[0])
    w_load.start()

    @pl.loop(0, THIRD)
    def _(q):
        o_send(q).start()

    @pl.when(diag)
    def _():
        cp = pltpu.make_async_copy(xt_ref, xv, aux.at[1])
        cp.start()

        @pl.when(z < N - 1)
        def _():
            x_up(xt_ref, 0).start()

        @pl.when(z > 0)
        def _():
            x_dn(xt_ref, 0).start()

        cp.wait()
        pltpu.make_async_copy(xv, xg_ref.at[0], aux.at[1]).start()

    w_load.wait()

    dist = jnp.abs(z - r)
    lag = jnp.where(z > r, N - 1 - z, jnp.where(z < r, z, jnp.maximum(z, N - 1 - z)))

    def x_step(c):
        for m in range(N):
            pos = jnp.where(dist == 0, 2 + m if m else -1, 3 * (m + dist))

            @pl.when(c == pos)
            def _():
                x_send_like = far(xt_ref, xg_ref.at[m], x_s.at[0], x_r.at[m], r=z)
                x_send_like.wait_recv()

                @pl.when(has_up)
                def _():
                    x_up(xg_ref.at[m], m).start()

                @pl.when(has_dn)
                def _():
                    x_dn(xg_ref.at[m], m).start()

    def f_step(q):
        y_send(q).wait_recv()
        f_send(q).start()

    def multiply(c, src0, src1):
        c0 = pltpu.make_async_copy(src0, dyv.at[pl.ds(0, p)], ld.at[0])
        c1 = pltpu.make_async_copy(src1, dyv.at[pl.ds(p, p)], ld.at[1])
        c0.start()
        c1.start()
        c0.wait()
        c1.wait()

        def part(i):
            s = pl.ds(pl.multiple_of(i * kb, kb), kb)
            return lax.dot_general(dyv[:, s], wv[:, s], (((1,), (1,)), ((), ())),
                                   preferred_element_type=jnp.float32)

        pv[c] = part(0)

        @pl.loop(1, 7)
        def _(i):
            pv[c] += part(i)

    def c_dn(c):
        return far(pv.at[c], upv.at[c], c_s.at[c], cu_r.at[c], c=z - 1)

    def c_up(c):
        return far(pv.at[c], dnv.at[c], c_s.at[c], cd_r.at[c], c=z + 1)

    def back(c, h, q, peer):
        return far(ov.at[c, pl.ds(h * p, p)], dx_ref.at[piece(q)], b_s.at[c, h], b_r.at[q], r=peer)

    def own_out(c):
        return pltpu.make_async_copy(ov.at[c], dx_ref.at[piece(2 * c, 2)], b_s.at[c, 0])

    def finish(c, start):
        def go(cp):
            if start:
                cp.start()
            else:
                cp.wait_send()

        @pl.when(c < THIRD)
        def _():
            if start:
                own_out(c).start()
            else:
                own_out(c).wait()

        @pl.when(jnp.logical_and(c >= THIRD, c < PIECES))
        def _():
            go(back(c, 0, 2 * (c - THIRD), r1))
            go(back(c, 1, 2 * (c - THIRD) + 1, r1))

        @pl.when(c >= PIECES)
        def _():
            go(back(c, 0, c - PIECES, r2))
            go(back(c, 1, c - PIECES, r3))

    def sum_step(c):
        @pl.when(has_up)
        def _():
            c_dn(c).wait_recv()
            pv[c] += upv[c]

        @pl.when(has_dn)
        def _():
            c_up(c).wait_recv()
            pv[c] += dnv[c]

        @pl.when(z > r)
        def _():
            c_dn(c).start()

        @pl.when(z < r)
        def _():
            c_up(c).start()

        @pl.when(diag)
        def _():
            ov[c] = pv[c].astype(jnp.bfloat16)
            finish(c, True)

    def after(c):
        x_step(c)

        @pl.when(c >= lag)
        def _():
            sum_step(c - lag)

    @pl.loop(0, PIECES)
    def _(c):
        @pl.when(jnp.logical_and(c >= 6, c % 2 == 0))
        def _():
            f_step((c - 6) // 2)

        @pl.when(c < THIRD)
        def _():
            multiply(c, dy_ref.at[piece(2 * c)], dy_ref.at[piece(2 * c + 1)])

        @pl.when(c >= THIRD)
        def _():
            i = c - THIRD
            o_send(i).wait_recv()
            multiply(c, dyg_ref.at[0, piece(2 * i)], dyg_ref.at[0, piece(2 * i + 1)])

        after(c)

    @pl.loop(PIECES, CHUNKS)
    def _(c):
        q = c - PIECES

        @pl.when(jnp.logical_and(c < 18, c % 2 == 0))
        def _():
            f_step((c - 6) // 2)

        @pl.when(c >= 18)
        def _():
            f_step(q)

        f_send(q).wait_recv()
        multiply(c, dyg_ref.at[1, piece(q)], dyg_ref.at[2, piece(q)])
        after(c)

    @pl.loop(0, N - 1)
    def _(i):
        @pl.when(i < lag)
        def _():
            sum_step(CHUNKS - lag + i)

    @pl.when(jnp.logical_not(diag))
    def _():
        x_send().wait_send()

        @pl.loop(0, CHUNKS)
        def _(c):
            c_dn(c).wait_send()

        @pl.loop(0, PIECES)
        def _(q):
            back(0, 0, q, r1).wait_recv()

    @pl.when(diag)
    def _():
        pltpu.make_async_copy(xv, xg_ref.at[0], aux.at[1]).wait()

        @pl.loop(0, CHUNKS)
        def _(c):
            finish(c, False)

    for m in range(N):
        @pl.when(has_up)
        def _():
            x_up(xg_ref.at[m], m).wait_send()

        @pl.when(has_dn)
        def _():
            x_dn(xg_ref.at[m], m).wait_send()

    @pl.loop(0, PIECES)
    def _(q):
        y_send(q).wait_send()
        f_send(q).wait_send()

    @pl.loop(0, THIRD)
    def _(q):
        o_send(q).wait_send()


def weight_grad(xg, dy, dyg):
    rows, n = dy.shape
    k = xg.shape[1]
    bn = n // 14

    def body(x_ref, d_ref, g_ref, o_ref):
        tot = jnp.dot(x_ref[0], d_ref[...], preferred_element_type=jnp.float32)
        for m in range(1, N):
            tot += jnp.dot(x_ref[m], g_ref[m - 1], preferred_element_type=jnp.float32)
        o_ref[...] = tot

    return pl.pallas_call(
        body,
        grid=(n // bn,),
        in_specs=[pl.BlockSpec(xg.shape, lambda i: (0, 0, 0)),
                  pl.BlockSpec((rows, bn), lambda i: (0, i)),
                  pl.BlockSpec((N - 1, rows, bn), lambda i: (0, 0, i))],
        out_specs=pl.BlockSpec((k, bn), lambda i: (0, i)),
        out_shape=jax.ShapeDtypeStruct((k, n), jnp.float32),
        compiler_params=pltpu.CompilerParams(vmem_limit_bytes=48 << 20),
        cost_estimate=pl.CostEstimate(flops=2 * N * rows * k * n, bytes_accessed=8 * rows * n + 4 * k * n,
                                      transcendentals=0),
        name="weight_grad",
    )(xg, dy, dyg)


def solution(mesh):
    def local(x, w, dy):
        xt = x.T
        rows, n = dy.shape
        k = w.shape[0]
        p = rows // PIECES
        dma = pltpu.SemaphoreType.DMA
        bf, f32 = jnp.bfloat16, jnp.float32
        dx, dyg, xg = pl.pallas_call(
            exchange,
            in_specs=[ANY] * 3,
            out_specs=[ANY] * 3,
            out_shape=[jax.ShapeDtypeStruct((rows, k), bf),
                       jax.ShapeDtypeStruct((N - 1, rows, n), bf),
                       jax.ShapeDtypeStruct((N, k, rows), bf)],
            scratch_shapes=[
                pltpu.VMEM((k, n), bf), pltpu.VMEM((2 * p, n), bf),
                pltpu.VMEM((CHUNKS, 2 * p, k), f32), pltpu.VMEM((CHUNKS, 2 * p, k), f32),
                pltpu.VMEM((CHUNKS, 2 * p, k), f32), pltpu.VMEM((CHUNKS, 2 * p, k), bf), pltpu.VMEM((k, rows), bf),
                dma((1,)), dma((N,)), dma((N,)), dma((N,)),
                dma((PIECES,)), dma((PIECES,)), dma((THIRD,)), dma((THIRD,)), dma((PIECES,)), dma((PIECES,)),
                dma((CHUNKS,)), dma((CHUNKS,)), dma((CHUNKS,)), dma((CHUNKS, 2)), dma((PIECES,)), dma((2,)), dma((2,)),
            ],
            compiler_params=pltpu.CompilerParams(collective_id=0, has_side_effects=True, vmem_limit_bytes=67043328),
            cost_estimate=pl.CostEstimate(flops=8 * rows * k * n, bytes_accessed=16 * rows * n, transcendentals=0),
            name="exchange",
        )(xt, w, dy)
        return dx, weight_grad(xg, dy, dyg)

    act = P(("dp", "r"), "c")
    return jax.shard_map(local, mesh=mesh, in_specs=(act, P("r", "c"), act),
                         out_specs=(act, act), check_vma=False)
```

```python
import jax
import jax.numpy as jnp
from jax import lax
from jax.experimental import pallas as pl
from jax.experimental.pallas import tpu as pltpu
from jax.sharding import PartitionSpec as P

N = 4
ANY = pl.BlockSpec(memory_space=pl.ANY)
PIECES = 12
PARTS = PIECES + 1
CHUNKS = 2 * PIECES
LAST = CHUNKS - 1
THIRD = PIECES // 2
UNITS = 28
PER = 3


def exchange(xt_ref, w_ref, dy_ref, dx_ref, dyg_ref, xg_ref, dwp_ref,
             wv, dyv, pv, upv, dnv, ov, xr, db, ob,
             x_s, xu_s, xd_s, x_r, y_s, y_r, o_s, o_r, f_s, f_r, c_s, cu_r, cd_r, b_s, b_r, ld, u_s, v_s, aux):
    r = lax.axis_index("r")
    z = lax.axis_index("c")
    r1 = r + 1 - 2 * (r % 2)
    r2 = (r + 2) % N
    r3 = N - 1 - r
    mx = ((r // 2 + z // 2) % 2) * 2 + (r % 2 + z % 2) % 2
    diag = r == z
    has_up = jnp.logical_and(z >= r, z < N - 1)
    has_dn = jnp.logical_and(z <= r, z > 0)
    rows = dy_ref.shape[0]
    p = rows // PIECES
    n = w_ref.shape[1]
    kb = n // 7

    def far(src, dst, s, d, **where):
        return pltpu.make_async_remote_copy(src_ref=src, dst_ref=dst, send_sem=s, recv_sem=d, device_id=where,
                                            device_id_type=pl.DeviceIdType.MESH)

    def piece(q, cnt=1):
        return pl.ds(pl.multiple_of(q * p, p), cnt * p)

    def half(j):
        return pl.ds((PIECES - 1) * p + j * (p // 2), p // 2)

    def where_rows(q):
        return half(q - PIECES + 1) if isinstance(q, int) and q >= PIECES - 1 else piece(q)

    barrier = pltpu.get_barrier_semaphore()
    for peer in (r1, r2, r3):
        pl.semaphore_signal(barrier, inc=1, device_id={"r": peer}, device_id_type=pl.DeviceIdType.MESH)

    @pl.when(z > 0)
    def _():
        pl.semaphore_signal(barrier, inc=1, device_id={"c": z - 1}, device_id_type=pl.DeviceIdType.MESH)

    @pl.when(z < N - 1)
    def _():
        pl.semaphore_signal(barrier, inc=1, device_id={"c": z + 1}, device_id_type=pl.DeviceIdType.MESH)

    pl.semaphore_wait(barrier, jnp.where(jnp.logical_or(z == 0, z == N - 1), 4, 5))

    def x_send():
        return far(xt_ref, xg_ref.at[mx], x_s.at[0], x_r.at[mx], r=z)

    def x_up(src, m):
        return far(src, xg_ref.at[m], xu_s.at[m], x_r.at[m], c=z + 1)

    def x_dn(src, m):
        return far(src, xg_ref.at[m], xd_s.at[m], x_r.at[m], c=z - 1)

    @pl.when(jnp.logical_not(diag))
    def _():
        x_send().start()

    def y_send(q):
        return far(dy_ref.at[where_rows(q)], dyg_ref.at[1, where_rows(q)], y_s.at[q], y_r.at[q], r=r2)

    def o_send(q):
        return far(dy_ref.at[piece(2 * q, 2)], dyg_ref.at[0, piece(2 * q, 2)], o_s.at[q], o_r.at[q], r=r1)

    def f_send(q):
        return far(dyg_ref.at[1, where_rows(q)], dyg_ref.at[2, where_rows(q)], f_s.at[q], f_r.at[q], r=r1)

    @pl.loop(0, PIECES - 1)
    def _(q):
        y_send(q).start()

    for q in (PIECES - 1, PIECES):
        y_send(q).start()

    w_load = pltpu.make_async_copy(w_ref, wv, aux.at[0])
    w_load.start()

    @pl.loop(0, THIRD)
    def _(q):
        o_send(q).start()

    @pl.when(diag)
    def _():
        cp = pltpu.make_async_copy(xt_ref, xr.at[:, pl.ds(0, rows)], aux.at[1])
        cp.start()

        @pl.when(z < N - 1)
        def _():
            x_up(xt_ref, 0).start()

        @pl.when(z > 0)
        def _():
            x_dn(xt_ref, 0).start()

        cp.wait()
        cp = pltpu.make_async_copy(xr.at[:, pl.ds(0, rows)], xg_ref.at[0], aux.at[1])
        cp.start()
        cp.wait()

    w_load.wait()

    dist = jnp.abs(z - r)
    lag = jnp.where(z > r, N - 1 - z, jnp.where(z < r, z, jnp.maximum(z, N - 1 - z)))

    def x_step(c):
        for m in range(N):
            pos = jnp.where(dist == 0, (-1, 3, 6, 7)[m], 3 * (m + dist) + (2 if m > 1 else -1))

            @pl.when(c == pos)
            def _():
                x_send_like = far(xt_ref, xg_ref.at[m], x_s.at[0], x_r.at[m], r=z)
                x_send_like.wait_recv()

                @pl.when(has_up)
                def _():
                    x_up(xg_ref.at[m], m).start()

                @pl.when(has_dn)
                def _():
                    x_dn(xg_ref.at[m], m).start()

    def f_step(q):
        y_send(q).wait_recv()
        f_send(q).start()

    def load_pair(i):
        return pltpu.make_async_copy(dy_ref.at[piece(4 * i, 4)], dyv, ld.at[0])

    def load_other(i):
        return pltpu.make_async_copy(dyg_ref.at[0, piece(4 * i, 4)], dyv, ld.at[0])

    def load_far(q, size):
        return [pltpu.make_async_copy(dyg_ref.at[1 + h, where_rows(q)], dyv.at[pl.ds(h * size, size)], ld.at[h])
                for h in (0, 1)]

    def product(dsts, size):
        def part(i):
            s = pl.ds(pl.multiple_of(i * kb, kb), kb)
            return lax.dot_general(dyv[:len(dsts) * size, s], wv[:, s], (((1,), (1,)), ((), ())),
                                   preferred_element_type=jnp.float32)

        first = part(0)
        for j, d in enumerate(dsts):
            d[...] = first[j * size:(j + 1) * size]

        @pl.loop(1, 7)
        def _(i):
            t = part(i)
            for j, d in enumerate(dsts):
                d[...] += t[j * size:(j + 1) * size]

    def rows_of(ref, c):
        if isinstance(c, int) and c >= LAST:
            return ref.at[LAST, pl.ds((c - LAST) * p, p)]
        return ref.at[c]

    def by_size(c, fn):
        @pl.when(c < LAST)
        def _():
            fn(c)

        for j in (LAST, LAST + 1):
            @pl.when(c == j)
            def _():
                fn(j)

    def c_dn(c):
        return far(rows_of(pv, c), rows_of(upv, c), c_s.at[c], cu_r.at[c], c=z - 1)

    def c_up(c):
        return far(rows_of(pv, c), rows_of(dnv, c), c_s.at[c], cd_r.at[c], c=z + 1)

    def back(c, h, q, peer, off, size):
        return far(ov.at[min(c, LAST) if isinstance(c, int) else c, pl.ds(off, size)], dx_ref.at[where_rows(q)],
                   b_s.at[c, h], b_r.at[q], r=peer)

    def own_out(c):
        return pltpu.make_async_copy(ov.at[c], dx_ref.at[piece(2 * c, 2)], b_s.at[c, 0])

    def finish(c, start):
        def go(cp):
            if start:
                cp.start()
            else:
                cp.wait_send()

        if isinstance(c, int):
            q, off, h = c - PIECES, (c - LAST) * p, p // 2
            go(back(c, 0, q, r2, off, h))
            go(back(c, 1, q, r3, off + h, h))
            return

        @pl.when(c < THIRD)
        def _():
            if start:
                own_out(c).start()
            else:
                own_out(c).wait()

        @pl.when(jnp.logical_and(c >= THIRD, c < PIECES - 1))
        def _():
            go(back(c, 0, 2 * (c - THIRD), r1, 0, p))
            go(back(c, 1, 2 * (c - THIRD) + 1, r1, p, p))

        @pl.when(c == PIECES - 1)
        def _():
            go(back(PIECES - 1, 0, PIECES - 2, r1, 0, p))
            go(back(PIECES - 1, 1, PIECES - 1, r1, p, p // 2))
            go(back(PIECES - 1, 2, PIECES, r1, p + p // 2, p // 2))

        @pl.when(c >= PIECES)
        def _():
            go(back(c, 0, c - PIECES, r2, 0, p))
            go(back(c, 1, c - PIECES, r3, p, p))

    def sum_one(c):
        mine = rows_of(pv, c)

        @pl.when(has_up)
        def _():
            c_dn(c).wait_recv()
            mine[...] += rows_of(upv, c)[...]

        @pl.when(has_dn)
        def _():
            c_up(c).wait_recv()
            mine[...] += rows_of(dnv, c)[...]

        @pl.when(z > r)
        def _():
            c_dn(c).start()

        @pl.when(z < r)
        def _():
            c_up(c).start()

        @pl.when(diag)
        def _():
            rows_of(ov, c)[...] = mine[...].astype(jnp.bfloat16)
            finish(c, True)

    def sum_step(c):
        by_size(c, sum_one)

    ub = n // UNITS
    spans = ((0, rows), (rows, rows))

    def xr_load(m):
        o, cnt = spans[m]
        return pltpu.make_async_copy(xg_ref.at[m, :, pl.ds(0, cnt)], xr.at[:, pl.ds(o, cnt)], v_s.at[m])

    def unit_load(u, m):
        o, cnt = spans[m]
        cols = pl.ds(pl.multiple_of(u * ub, ub), ub)
        src = dy_ref.at[:, cols] if m == 0 else dyg_ref.at[m - 1, :, cols]
        return pltpu.make_async_copy(src, db.at[u % 2, pl.ds(o, cnt)], u_s.at[u % 2, m])

    def unit_out(u):
        cols = pl.ds(pl.multiple_of(u * ub, ub), ub)
        return pltpu.make_async_copy(ob.at[u % 2], dwp_ref.at[:, cols], u_s.at[u % 2, 2])

    def unit(u):
        @pl.when(u == 0)
        def _():
            for m in range(2):
                xr_load(m).start()
                unit_load(0, m).start()
            for m in range(2):
                xr_load(m).wait()

        @pl.when(u + 1 < UNITS)
        def _():
            for m in range(2):
                unit_load(u + 1, m).start()

        for m in range(2):
            unit_load(u, m).wait()

        @pl.when(u >= 2)
        def _():
            unit_out(u - 2).wait()

        ob[u % 2] = jnp.dot(xr[...], db[u % 2], preferred_element_type=jnp.float32)
        unit_out(u).start()

    def after(c):
        @pl.when(c >= lag)
        def _():
            sum_step(c - lag)

    base = jnp.where(r // 2 == z // 2, 6, 3)
    ahead = PIECES - base

    def f_early(c):
        @pl.when(jnp.logical_and(c >= base, (c - base) % 2 == 0))
        def _():
            q = (c - base) // 2

            @pl.when(q <= ahead)
            def _():
                f_step(q)

    u0 = jnp.where(dist == 0, 4, 3 * (1 + dist))

    def units(c):
        @pl.when(c >= u0)
        def _():
            @pl.loop(0, PER)
            def _(i):
                u = (c - u0) * PER + i

                @pl.when(u < UNITS)
                def _():
                    unit(u)

    load_pair(0).start()

    @pl.loop(0, THIRD)
    def _(i):
        c = 2 * i
        f_early(c)
        load_pair(0).wait()
        product([pv.at[c], pv.at[c + 1]], 2 * p)

        @pl.when(i + 1 < THIRD // 2)
        def _():
            load_pair(i + 1).start()

        @pl.when(jnp.logical_and(i + 1 >= THIRD // 2, i + 1 < THIRD))
        def _():
            k = i + 1 - THIRD // 2

            @pl.when(k == 0)
            def _():
                @pl.loop(0, THIRD)
                def _(q):
                    o_send(q).wait_recv()

            load_other(k).start()

        x_step(c)
        after(c)
        units(c)
        f_early(c + 1)
        x_step(c + 1)
        after(c + 1)
        units(c + 1)

    @pl.loop(PIECES, LAST)
    def _(c):
        q = c - PIECES
        f_early(c)

        @pl.when(q > ahead)
        def _():
            f_step(q)

        f_send(q).wait_recv()
        for cp in load_far(q, p):
            cp.start()
        for cp in load_far(q, p):
            cp.wait()
        product([pv.at[c]], 2 * p)
        x_step(c)
        after(c)
        units(c)

    for c in (LAST, LAST + 1):
        q = c - PIECES
        f_step(q)
        f_send(q).wait_recv()
        for cp in load_far(q, p // 2):
            cp.start()
        for cp in load_far(q, p // 2):
            cp.wait()
        product([rows_of(pv, c)], p)
        sum_step(c - lag)

    @pl.loop(0, N - 1)
    def _(i):
        @pl.when(i < lag)
        def _():
            sum_step(CHUNKS + 1 - lag + i)

    for u in (UNITS - 2, UNITS - 1):
        unit_out(u).wait()

    @pl.when(jnp.logical_not(diag))
    def _():
        x_send().wait_send()

        @pl.loop(0, LAST)
        def _(c):
            c_dn(c).wait_send()

        for c in (LAST, LAST + 1):
            c_dn(c).wait_send()

        @pl.loop(0, PIECES - 1)
        def _(q):
            back(0, 0, q, r1, 0, p).wait_recv()

        for q in (PIECES - 1, PIECES):
            back(0, 0, q, r1, 0, p // 2).wait_recv()

    @pl.when(diag)
    def _():
        @pl.loop(0, LAST)
        def _(c):
            finish(c, False)

        for c in (LAST, LAST + 1):
            finish(c, False)

    for m in range(N):
        @pl.when(has_up)
        def _():
            x_up(xg_ref.at[m], m).wait_send()

        @pl.when(has_dn)
        def _():
            x_dn(xg_ref.at[m], m).wait_send()

    @pl.loop(0, PIECES - 1)
    def _(q):
        y_send(q).wait_send()
        f_send(q).wait_send()

    for q in (PIECES - 1, PIECES):
        y_send(q).wait_send()
        f_send(q).wait_send()

    @pl.loop(0, THIRD)
    def _(q):
        o_send(q).wait_send()


BLOCKS = 14
SLOTS = 6


def finish_grads(xg_ref, dyg_ref, dwp_ref, dxp_ref, dw_ref, dx_ref, xr, db, ob, dv, x_s, l_s, o_s, d_s):
    rows = dyg_ref.shape[1]
    bn = dw_ref.shape[1] // BLOCKS
    ahead = SLOTS - 2

    def load(u, h):
        cols, s = pl.ds(pl.multiple_of(u * bn, bn), bn), lax.rem(u, SLOTS)
        if h == 2:
            return pltpu.make_async_copy(dwp_ref.at[:, cols], ob.at[s], l_s.at[s, 2])
        return pltpu.make_async_copy(dyg_ref.at[1 + h, :, cols], db.at[s, pl.ds(h * rows, rows)], l_s.at[s, h])

    def out(u):
        cols, s = pl.ds(pl.multiple_of(u * bn, bn), bn), lax.rem(u, SLOTS)
        return pltpu.make_async_copy(ob.at[s], dw_ref.at[:, cols], o_s.at[s])

    xs = [pltpu.make_async_copy(xg_ref.at[2 + h], xr.at[:, pl.ds(h * rows, rows)], x_s.at[h]) for h in (0, 1)]
    d_in = pltpu.make_async_copy(dxp_ref, dv, d_s.at[0])
    d_out = pltpu.make_async_copy(dv, dx_ref, d_s.at[1])
    for cp in xs:
        cp.start()

    @pl.loop(0, ahead)
    def _(u):
        for h in range(3):
            load(u, h).start()

    d_in.start()
    for cp in xs:
        cp.wait()

    @pl.loop(0, BLOCKS)
    def _(u):
        @pl.when(u >= 2)
        def _():
            out(u - 2).wait()

        @pl.when(u + ahead < BLOCKS)
        def _():
            for h in range(3):
                load(u + ahead, h).start()

        for h in range(3):
            load(u, h).wait()
        s = lax.rem(u, SLOTS)
        ob[s] += jnp.dot(xr[...], db[s], preferred_element_type=jnp.float32)
        out(u).start()

        @pl.when(u == 2)
        def _():
            d_in.wait()
            d_out.start()

    out(BLOCKS - 2).wait()
    out(BLOCKS - 1).wait()
    d_out.wait()


def solution(mesh):
    def local(x, w, dy):
        xt = x.T
        rows, n = dy.shape
        k = w.shape[0]
        p = rows // PIECES
        dma = pltpu.SemaphoreType.DMA
        bf, f32 = jnp.bfloat16, jnp.float32
        dx, dyg, xg, dwp = pl.pallas_call(
            exchange,
            in_specs=[ANY] * 3,
            out_specs=[ANY] * 4,
            out_shape=[jax.ShapeDtypeStruct((rows, k), bf),
                       jax.ShapeDtypeStruct((N - 1, rows, n), bf),
                       jax.ShapeDtypeStruct((N, k, rows), bf),
                       jax.ShapeDtypeStruct((k, n), f32)],
            scratch_shapes=[
                pltpu.VMEM((k, n), bf), pltpu.VMEM((4 * p, n), bf),
                pltpu.VMEM((CHUNKS, 2 * p, k), f32), pltpu.VMEM((CHUNKS, 2 * p, k), f32),
                pltpu.VMEM((CHUNKS, 2 * p, k), f32), pltpu.VMEM((CHUNKS, 2 * p, k), bf),
                pltpu.VMEM((k, 2 * rows), bf),
                pltpu.VMEM((2, 2 * rows, n // UNITS), bf), pltpu.VMEM((2, k, n // UNITS), f32),
                dma((1,)), dma((N,)), dma((N,)), dma((N,)),
                dma((PARTS,)), dma((PARTS,)), dma((THIRD,)), dma((THIRD,)), dma((PARTS,)), dma((PARTS,)),
                dma((CHUNKS + 1,)), dma((CHUNKS + 1,)), dma((CHUNKS + 1,)), dma((CHUNKS + 1, 3)), dma((PARTS,)),
                dma((2,)), dma((2, 3)), dma((2,)), dma((2,)),
            ],
            compiler_params=pltpu.CompilerParams(collective_id=0, has_side_effects=True, vmem_limit_bytes=67043328),
            cost_estimate=pl.CostEstimate(flops=8 * rows * k * n, bytes_accessed=16 * rows * n, transcendentals=0),
            name="exchange",
        )(xt, w, dy)
        dw, dx = pl.pallas_call(
            finish_grads,
            in_specs=[ANY] * 4,
            out_specs=[ANY] * 2,
            out_shape=[jax.ShapeDtypeStruct((k, n), f32), jax.ShapeDtypeStruct((rows, k), bf)],
            scratch_shapes=[pltpu.VMEM((k, 2 * rows), bf), pltpu.VMEM((SLOTS, 2 * rows, n // BLOCKS), bf),
                            pltpu.VMEM((SLOTS, k, n // BLOCKS), f32), pltpu.VMEM((rows, k), bf),
                            dma((2,)), dma((SLOTS, 3)), dma((SLOTS,)), dma((2,))],
            compiler_params=pltpu.CompilerParams(vmem_limit_bytes=67043328),
            cost_estimate=pl.CostEstimate(flops=4 * rows * k * n, bytes_accessed=4 * rows * n + 8 * k * n,
                                          transcendentals=0),
            name="finish_grads",
        )(xg, dyg, dwp, dx)
        return dx, dw

    act = P(("dp", "r"), "c")
    return jax.shard_map(local, mesh=mesh, in_specs=(act, P("r", "c"), act),
                         out_specs=(act, act), check_vma=False)
```

```python
import jax
import jax.numpy as jnp
from jax import lax
from jax.experimental import pallas as pl
from jax.experimental.pallas import tpu as pltpu
from jax.sharding import PartitionSpec as P

N = 4
ANY = pl.BlockSpec(memory_space=pl.ANY)
PIECES = 12
PARTS = PIECES + 1
CHUNKS = 2 * PIECES
LAST = CHUNKS - 1
THIRD = PIECES // 2
UNITS = 28
PER = 4


def exchange(x_ref, w_ref, dy_ref, dx_ref, dyg_ref, xg_ref, dwp_ref, xt_ref,
             wv, dyv, pv, upv, dnv, ov, xr, db, ob,
             x_s, xu_s, xd_s, x_r, y_s, y_r, o_s, o_r, f_s, f_r, c_s, cu_r, cd_r, b_s, b_r, ld, u_s, v_s, aux):
    r = lax.axis_index("r")
    z = lax.axis_index("c")
    r1 = r + 1 - 2 * (r % 2)
    r2 = (r + 2) % N
    r3 = N - 1 - r
    mx = ((r // 2 + z // 2) % 2) * 2 + (r % 2 + z % 2) % 2
    diag = r == z
    has_up = jnp.logical_and(z >= r, z < N - 1)
    has_dn = jnp.logical_and(z <= r, z > 0)
    rows = dy_ref.shape[0]
    p = rows // PIECES
    n = w_ref.shape[1]

    def far(src, dst, s, d, **where):
        return pltpu.make_async_remote_copy(src_ref=src, dst_ref=dst, send_sem=s, recv_sem=d, device_id=where,
                                            device_id_type=pl.DeviceIdType.MESH)

    def piece(q, cnt=1):
        return pl.ds(pl.multiple_of(q * p, p), cnt * p)

    def half(j):
        return pl.ds((PIECES - 1) * p + j * (p // 2), p // 2)

    def where_rows(q):
        return half(q - PIECES + 1) if isinstance(q, int) and q >= PIECES - 1 else piece(q)

    barrier = pltpu.get_barrier_semaphore()
    for peer in (r1, r2, r3):
        pl.semaphore_signal(barrier, inc=1, device_id={"r": peer}, device_id_type=pl.DeviceIdType.MESH)

    @pl.when(z > 0)
    def _():
        pl.semaphore_signal(barrier, inc=1, device_id={"c": z - 1}, device_id_type=pl.DeviceIdType.MESH)

    @pl.when(z < N - 1)
    def _():
        pl.semaphore_signal(barrier, inc=1, device_id={"c": z + 1}, device_id_type=pl.DeviceIdType.MESH)

    pl.semaphore_wait(barrier, jnp.where(jnp.logical_or(z == 0, z == N - 1), 4, 5))

    def x_send():
        return far(xt_ref, xg_ref.at[mx], x_s.at[0], x_r.at[mx], r=z)

    def x_up(src, m):
        return far(src, xg_ref.at[m], xu_s.at[m], x_r.at[m], c=z + 1)

    def x_dn(src, m):
        return far(src, xg_ref.at[m], xd_s.at[m], x_r.at[m], c=z - 1)

    def y_send(q):
        return far(dy_ref.at[where_rows(q)], dyg_ref.at[1, where_rows(q)], y_s.at[q], y_r.at[q], r=r2)

    def o_send(q):
        return far(dy_ref.at[piece(2 * q, 2)], dyg_ref.at[0, piece(2 * q, 2)], o_s.at[q], o_r.at[q], r=r1)

    def f_send(q):
        return far(dyg_ref.at[1, where_rows(q)], dyg_ref.at[2, where_rows(q)], f_s.at[q], f_r.at[q], r=r1)

    y_send(0).start()
    x_rows = x_ref.shape[0]
    x_load = pltpu.make_async_copy(x_ref, ov.at[pl.ds(0, x_rows)], aux.at[1])
    x_load.start()
    w_load = pltpu.make_async_copy(w_ref, wv, aux.at[0])
    w_load.start()
    x_load.wait()
    for j in range(x_rows):
        xr[:, pl.ds(j * 2 * p, 2 * p)] = ov[j].T
    x_store = pltpu.make_async_copy(xr.at[:, pl.ds(0, rows)], xt_ref, aux.at[1])
    x_store.start()
    x_store.wait()

    @pl.when(jnp.logical_not(diag))
    def _():
        x_send().start()

    @pl.loop(1, PIECES - 1)
    def _(q):
        y_send(q).start()

    for q in (PIECES - 1, PIECES):
        y_send(q).start()

    @pl.loop(0, THIRD)
    def _(q):
        o_send(q).start()

    @pl.when(diag)
    def _():
        @pl.when(z < N - 1)
        def _():
            x_up(xt_ref, 0).start()

        @pl.when(z > 0)
        def _():
            x_dn(xt_ref, 0).start()

        cp = pltpu.make_async_copy(xr.at[:, pl.ds(0, rows)], xg_ref.at[0], aux.at[1])
        cp.start()
        cp.wait()

    w_load.wait()

    dist = jnp.abs(z - r)
    lag = jnp.where(z > r, N - 1 - z, jnp.where(z < r, z, jnp.maximum(z, N - 1 - z)))

    def x_step(c):
        for m in range(N):
            pos = jnp.where(dist == 0, (-1, 3, 6, 7)[m], 3 * (m + dist) - 1)

            @pl.when(c == pos)
            def _():
                x_send_like = far(xt_ref, xg_ref.at[m], x_s.at[0], x_r.at[m], r=z)
                x_send_like.wait_recv()

                @pl.when(has_up)
                def _():
                    x_up(xg_ref.at[m], m).start()

                @pl.when(has_dn)
                def _():
                    x_dn(xg_ref.at[m], m).start()

    def f_step(q):
        y_send(q).wait_recv()
        f_send(q).start()

    def load_pair(i):
        return pltpu.make_async_copy(dy_ref.at[piece(4 * i, 4)], dyv, ld.at[0])

    def load_other(i):
        return pltpu.make_async_copy(dyg_ref.at[0, piece(4 * i, 4)], dyv, ld.at[0])

    def load_far(q, size):
        return [pltpu.make_async_copy(dyg_ref.at[1 + h, where_rows(q)], dyv.at[pl.ds(h * size, size)], ld.at[h])
                for h in (0, 1)]

    def product(dsts, size):
        t = lax.dot_general(dyv[:len(dsts) * size], wv[...], (((1,), (1,)), ((), ())),
                            preferred_element_type=jnp.float32)
        for j, d in enumerate(dsts):
            d[...] = t[j * size:(j + 1) * size]

    def rows_of(ref, c):
        if isinstance(c, int) and c >= LAST:
            return ref.at[LAST, pl.ds((c - LAST) * p, p)]
        return ref.at[c]

    def by_size(c, fn):
        @pl.when(c < LAST)
        def _():
            fn(c)

        for j in (LAST, LAST + 1):
            @pl.when(c == j)
            def _():
                fn(j)

    def c_dn(c):
        return far(rows_of(pv, c), rows_of(upv, c), c_s.at[c], cu_r.at[c], c=z - 1)

    def c_up(c):
        return far(rows_of(pv, c), rows_of(dnv, c), c_s.at[c], cd_r.at[c], c=z + 1)

    def back(c, h, q, peer, off, size):
        return far(ov.at[min(c, LAST) if isinstance(c, int) else c, pl.ds(off, size)], dx_ref.at[where_rows(q)],
                   b_s.at[c, h], b_r.at[q], r=peer)

    def own_out(c):
        return pltpu.make_async_copy(ov.at[c], dx_ref.at[piece(2 * c, 2)], b_s.at[c, 0])

    def finish(c, start):
        def go(cp):
            if start:
                cp.start()
            else:
                cp.wait_send()

        if isinstance(c, int):
            q, off, h = c - PIECES, (c - LAST) * p, p // 2
            go(back(c, 0, q, r2, off, h))
            go(back(c, 1, q, r3, off + h, h))
            return

        @pl.when(c < THIRD)
        def _():
            if start:
                own_out(c).start()
            else:
                own_out(c).wait()

        @pl.when(jnp.logical_and(c >= THIRD, c < PIECES - 1))
        def _():
            go(back(c, 0, 2 * (c - THIRD), r1, 0, p))
            go(back(c, 1, 2 * (c - THIRD) + 1, r1, p, p))

        @pl.when(c == PIECES - 1)
        def _():
            go(back(PIECES - 1, 0, PIECES - 2, r1, 0, p))
            go(back(PIECES - 1, 1, PIECES - 1, r1, p, p // 2))
            go(back(PIECES - 1, 2, PIECES, r1, p + p // 2, p // 2))

        @pl.when(c >= PIECES)
        def _():
            go(back(c, 0, c - PIECES, r2, 0, p))
            go(back(c, 1, c - PIECES, r3, p, p))

    def sum_one(c):
        mine = rows_of(pv, c)

        @pl.when(has_up)
        def _():
            c_dn(c).wait_recv()
            mine[...] += rows_of(upv, c)[...]

        @pl.when(has_dn)
        def _():
            c_up(c).wait_recv()
            mine[...] += rows_of(dnv, c)[...]

        @pl.when(z > r)
        def _():
            c_dn(c).start()

        @pl.when(z < r)
        def _():
            c_up(c).start()

        @pl.when(diag)
        def _():
            rows_of(ov, c)[...] = mine[...].astype(jnp.bfloat16)
            finish(c, True)

    def sum_step(c):
        by_size(c, sum_one)

    ub = n // UNITS
    spans = ((0, rows), (rows, rows))

    def xr_load(m):
        o, cnt = spans[m]
        return pltpu.make_async_copy(xg_ref.at[m, :, pl.ds(0, cnt)], xr.at[:, pl.ds(o, cnt)], v_s.at[m])

    def unit_load(u, m):
        o, cnt = spans[m]
        cols = pl.ds(pl.multiple_of(u * ub, ub), ub)
        src = dy_ref.at[:, cols] if m == 0 else dyg_ref.at[m - 1, :, cols]
        return pltpu.make_async_copy(src, db.at[u % 2, pl.ds(o, cnt)], u_s.at[u % 2, m])

    def unit_out(u):
        cols = pl.ds(pl.multiple_of(u * ub, ub), ub)
        return pltpu.make_async_copy(ob.at[u % 2], dwp_ref.at[:, cols], u_s.at[u % 2, 2])

    def unit(u):
        @pl.when(u == 0)
        def _():
            for m in range(2):
                xr_load(m).start()
                unit_load(0, m).start()
            for m in range(2):
                xr_load(m).wait()

        @pl.when(u + 1 < UNITS)
        def _():
            for m in range(2):
                unit_load(u + 1, m).start()

        for m in range(2):
            unit_load(u, m).wait()

        @pl.when(u >= 2)
        def _():
            unit_out(u - 2).wait()

        ob[u % 2] = jnp.dot(xr[...], db[u % 2], preferred_element_type=jnp.float32)
        unit_out(u).start()

    end_lag = jnp.where(diag, jnp.minimum(lag, 1), 0)
    gap = lag - end_lag
    mid_lag = jnp.where(gap >= 1, lag - 1, lag)

    def after(c):
        now = jnp.where(c == LAST - 1, mid_lag, lag)

        @pl.when(c >= now)
        def _():
            sum_step(c - now)

        @pl.when(jnp.logical_or(jnp.logical_and(c == LAST - 2, gap >= 1), jnp.logical_and(c == LAST - 1, gap >= 2)))
        def _():
            sum_one(c + 1 - now)

    base = jnp.where(r // 2 == z // 2, 6, 3)
    ahead = PIECES - base

    def f_early(c):
        @pl.when(jnp.logical_and(c >= base, (c - base) % 2 == 0))
        def _():
            q = (c - base) // 2

            @pl.when(q <= ahead)
            def _():
                f_step(q)

    u0 = jnp.where(dist == 0, 4, 3 * (1 + dist))

    def units(c):
        @pl.when(c >= u0)
        def _():
            @pl.loop(0, PER)
            def _(i):
                u = (c - u0) * PER + i

                @pl.when(u < UNITS)
                def _():
                    unit(u)

    load_pair(0).start()

    @pl.loop(0, THIRD)
    def _(i):
        c = 2 * i
        f_early(c)
        load_pair(0).wait()
        product([pv.at[c], pv.at[c + 1]], 2 * p)

        @pl.when(i + 1 < THIRD // 2)
        def _():
            load_pair(i + 1).start()

        @pl.when(jnp.logical_and(i + 1 >= THIRD // 2, i + 1 < THIRD))
        def _():
            k = i + 1 - THIRD // 2

            @pl.when(k == 0)
            def _():
                @pl.loop(0, THIRD)
                def _(q):
                    o_send(q).wait_recv()

            load_other(k).start()

        x_step(c)
        after(c)
        units(c)
        f_early(c + 1)
        x_step(c + 1)
        after(c + 1)
        units(c + 1)

    @pl.loop(PIECES, LAST)
    def _(c):
        q = c - PIECES
        f_early(c)

        @pl.when(q > ahead)
        def _():
            f_step(q)

        f_send(q).wait_recv()
        for cp in load_far(q, p):
            cp.start()
        for cp in load_far(q, p):
            cp.wait()
        product([pv.at[c]], 2 * p)
        x_step(c)
        after(c)
        units(c)

    for c in (LAST, LAST + 1):
        q = c - PIECES
        f_step(q)
        f_send(q).wait_recv()
        for cp in load_far(q, p // 2):
            cp.start()
        for cp in load_far(q, p // 2):
            cp.wait()
        product([rows_of(pv, c)], p)
        sum_step(c - end_lag)

    @pl.when(end_lag == 1)
    def _():
        sum_one(LAST + 1)

    for u in (UNITS - 2, UNITS - 1):
        unit_out(u).wait()

    @pl.when(jnp.logical_not(diag))
    def _():
        x_send().wait_send()

        @pl.loop(0, LAST)
        def _(c):
            c_dn(c).wait_send()

        for c in (LAST, LAST + 1):
            c_dn(c).wait_send()

        @pl.loop(0, PIECES - 1)
        def _(q):
            back(0, 0, q, r1, 0, p).wait_recv()

        for q in (PIECES - 1, PIECES):
            back(0, 0, q, r1, 0, p // 2).wait_recv()

    @pl.when(diag)
    def _():
        @pl.loop(0, LAST)
        def _(c):
            finish(c, False)

        for c in (LAST, LAST + 1):
            finish(c, False)

    for m in range(N):
        @pl.when(has_up)
        def _():
            x_up(xg_ref.at[m], m).wait_send()

        @pl.when(has_dn)
        def _():
            x_dn(xg_ref.at[m], m).wait_send()

    @pl.loop(0, PIECES - 1)
    def _(q):
        y_send(q).wait_send()
        f_send(q).wait_send()

    for q in (PIECES - 1, PIECES):
        y_send(q).wait_send()
        f_send(q).wait_send()

    @pl.loop(0, THIRD)
    def _(q):
        o_send(q).wait_send()


BLOCKS = 14
SLOTS = 6


def finish_grads(xg_ref, dyg_ref, dwp_ref, dxp_ref, dw_ref, dx_ref, xr, db, ob, dv, x_s, l_s, o_s, d_s):
    rows = dyg_ref.shape[1]
    bn = dw_ref.shape[1] // BLOCKS
    ahead = SLOTS - 2

    def load(u, h):
        cols, s = pl.ds(pl.multiple_of(u * bn, bn), bn), lax.rem(u, SLOTS)
        if h == 2:
            return pltpu.make_async_copy(dwp_ref.at[:, cols], ob.at[s], l_s.at[s, 2])
        return pltpu.make_async_copy(dyg_ref.at[1 + h, :, cols], db.at[s, pl.ds(h * rows, rows)], l_s.at[s, h])

    def out(u):
        cols, s = pl.ds(pl.multiple_of(u * bn, bn), bn), lax.rem(u, SLOTS)
        return pltpu.make_async_copy(ob.at[s], dw_ref.at[:, cols], o_s.at[s])

    xs = [pltpu.make_async_copy(xg_ref.at[2 + h], xr.at[:, pl.ds(h * rows, rows)], x_s.at[h])
          for h in (0, 1)]
    d_in = pltpu.make_async_copy(dxp_ref, dv, d_s.at[0])
    d_out = pltpu.make_async_copy(dv, dx_ref, d_s.at[1])
    for cp in xs:
        cp.start()

    @pl.loop(0, ahead)
    def _(u):
        for h in range(3):
            load(u, h).start()

    d_in.start()
    for cp in xs:
        cp.wait()

    @pl.loop(0, BLOCKS)
    def _(u):
        @pl.when(u >= 2)
        def _():
            out(u - 2).wait()

        @pl.when(u + ahead < BLOCKS)
        def _():
            for h in range(3):
                load(u + ahead, h).start()

        for h in range(3):
            load(u, h).wait()
        s = lax.rem(u, SLOTS)
        ob[s] += jnp.dot(xr[...], db[s], preferred_element_type=jnp.float32)
        out(u).start()

        @pl.when(u == 2)
        def _():
            d_in.wait()
            d_out.start()

    out(BLOCKS - 2).wait()
    out(BLOCKS - 1).wait()
    d_out.wait()


def solution(mesh):
    def local(x, w, dy):
        rows, n = dy.shape
        k = w.shape[0]
        p = rows // PIECES
        dma = pltpu.SemaphoreType.DMA
        bf, f32 = jnp.bfloat16, jnp.float32
        dx, dyg, xg, dwp, _ = pl.pallas_call(
            exchange,
            in_specs=[ANY] * 3,
            out_specs=[ANY] * 5,
            out_shape=[jax.ShapeDtypeStruct((rows, k), bf),
                       jax.ShapeDtypeStruct((N - 1, rows, n), bf),
                       jax.ShapeDtypeStruct((N, k, rows), bf),
                       jax.ShapeDtypeStruct((k, n), f32),
                       jax.ShapeDtypeStruct((k, rows), bf)],
            scratch_shapes=[
                pltpu.VMEM((k, n), bf), pltpu.VMEM((4 * p, n), bf),
                pltpu.VMEM((CHUNKS, 2 * p, k), f32), pltpu.VMEM((CHUNKS, 2 * p, k), f32),
                pltpu.VMEM((CHUNKS, 2 * p, k), f32), pltpu.VMEM((CHUNKS, 2 * p, k), bf),
                pltpu.VMEM((k, 2 * rows), bf),
                pltpu.VMEM((2, 2 * rows, n // UNITS), bf), pltpu.VMEM((2, k, n // UNITS), f32),
                dma((1,)), dma((N,)), dma((N,)), dma((N,)),
                dma((PARTS,)), dma((PARTS,)), dma((THIRD,)), dma((THIRD,)), dma((PARTS,)), dma((PARTS,)),
                dma((CHUNKS + 1,)), dma((CHUNKS + 1,)), dma((CHUNKS + 1,)), dma((CHUNKS + 1, 3)), dma((PARTS,)),
                dma((2,)), dma((2, 3)), dma((2,)), dma((2,)),
            ],
            compiler_params=pltpu.CompilerParams(collective_id=0, has_side_effects=True, vmem_limit_bytes=67043328),
            cost_estimate=pl.CostEstimate(flops=8 * rows * k * n, bytes_accessed=16 * rows * n, transcendentals=0),
            name="exchange",
        )(x.reshape(rows // (2 * p), 2 * p, k), w, dy)
        dw, dx = pl.pallas_call(
            finish_grads,
            in_specs=[ANY] * 4,
            out_specs=[ANY] * 2,
            out_shape=[jax.ShapeDtypeStruct((k, n), f32), jax.ShapeDtypeStruct((rows, k), bf)],
            scratch_shapes=[pltpu.VMEM((k, 2 * rows), bf), pltpu.VMEM((SLOTS, 2 * rows, n // BLOCKS), bf),
                            pltpu.VMEM((SLOTS, k, n // BLOCKS), f32), pltpu.VMEM((rows, k), bf),
                            dma((2,)), dma((SLOTS, 3)), dma((SLOTS,)), dma((2,))],
            compiler_params=pltpu.CompilerParams(vmem_limit_bytes=67043328),
            cost_estimate=pl.CostEstimate(flops=4 * rows * k * n, bytes_accessed=4 * rows * n + 8 * k * n,
                                          transcendentals=0),
            name="finish_grads",
        )(xg, dyg, dwp, dx)
        return dx, dw

    act = P(("dp", "r"), "c")
    return jax.shard_map(local, mesh=mesh, in_specs=(act, P("r", "c"), act),
                         out_specs=(act, act), check_vma=False)
```

```python
import jax
import jax.numpy as jnp
from jax import lax
from jax.experimental import pallas as pl
from jax.experimental.pallas import tpu as pltpu
from jax.sharding import PartitionSpec as P

N = 4
ANY = pl.BlockSpec(memory_space=pl.ANY)
PIECES = 12
PARTS = PIECES + 1
CHUNKS = 2 * PIECES
LAST = CHUNKS - 1
THIRD = PIECES // 2
UNITS = 28
PER = 4


def exchange(x_ref, w_ref, dy_ref, dx_ref, dyg_ref, xg_ref, dwp_ref, xt_ref,
             wv, dyv, pv, upv, dnv, ov, xr, db, ob,
             x_s, xu_s, xd_s, x_r, y_s, y_r, o_s, o_r, f_s, f_r, c_s, cu_r, cd_r, b_s, b_r, ld, u_s, v_s, aux):
    r = lax.axis_index("r")
    z = lax.axis_index("c")
    r1 = r + 1 - 2 * (r % 2)
    r2 = (r + 2) % N
    r3 = N - 1 - r
    mx = ((r // 2 + z // 2) % 2) * 2 + (r % 2 + z % 2) % 2
    diag = r == z
    has_up = jnp.logical_and(z >= r, z < N - 1)
    has_dn = jnp.logical_and(z <= r, z > 0)
    rows = dy_ref.shape[0]
    p = rows // PIECES
    n = w_ref.shape[1]

    def far(src, dst, s, d, **where):
        return pltpu.make_async_remote_copy(src_ref=src, dst_ref=dst, send_sem=s, recv_sem=d, device_id=where,
                                            device_id_type=pl.DeviceIdType.MESH)

    def piece(q, cnt=1):
        return pl.ds(pl.multiple_of(q * p, p), cnt * p)

    def half(j):
        return pl.ds((PIECES - 1) * p + j * (p // 2), p // 2)

    def where_rows(q):
        return half(q - PIECES + 1) if isinstance(q, int) and q >= PIECES - 1 else piece(q)

    barrier = pltpu.get_barrier_semaphore()
    for peer in (r1, r2, r3):
        pl.semaphore_signal(barrier, inc=1, device_id={"r": peer}, device_id_type=pl.DeviceIdType.MESH)

    @pl.when(z > 0)
    def _():
        pl.semaphore_signal(barrier, inc=1, device_id={"c": z - 1}, device_id_type=pl.DeviceIdType.MESH)

    @pl.when(z < N - 1)
    def _():
        pl.semaphore_signal(barrier, inc=1, device_id={"c": z + 1}, device_id_type=pl.DeviceIdType.MESH)

    pl.semaphore_wait(barrier, jnp.where(jnp.logical_or(z == 0, z == N - 1), 4, 5))

    def x_send():
        return far(xt_ref, xg_ref.at[mx], x_s.at[0], x_r.at[mx], r=z)

    def x_up(src, m):
        return far(src, xg_ref.at[m], xu_s.at[m], x_r.at[m], c=z + 1)

    def x_dn(src, m):
        return far(src, xg_ref.at[m], xd_s.at[m], x_r.at[m], c=z - 1)

    def y_send(q):
        return far(dy_ref.at[where_rows(q)], dyg_ref.at[1, where_rows(q)], y_s.at[q], y_r.at[q], r=r2)

    def o_send(q):
        return far(dy_ref.at[piece(2 * q, 2)], dyg_ref.at[0, piece(2 * q, 2)], o_s.at[q], o_r.at[q], r=r1)

    def f_send(q):
        return far(dyg_ref.at[1, where_rows(q)], dyg_ref.at[2, where_rows(q)], f_s.at[q], f_r.at[q], r=r1)

    y_send(0).start()
    x_rows = x_ref.shape[0]
    x_load = pltpu.make_async_copy(x_ref, ov.at[pl.ds(0, x_rows)], aux.at[1])
    x_load.start()
    w_load = pltpu.make_async_copy(w_ref, wv, aux.at[0])
    w_load.start()
    x_load.wait()
    for j in range(x_rows):
        xr[:, pl.ds(j * 2 * p, 2 * p)] = ov[j].T
    x_store = pltpu.make_async_copy(xr.at[:, pl.ds(0, rows)], xt_ref, aux.at[1])
    x_store.start()
    x_store.wait()

    @pl.when(jnp.logical_not(diag))
    def _():
        x_send().start()

    @pl.loop(1, PIECES - 1)
    def _(q):
        y_send(q).start()

    for q in (PIECES - 1, PIECES):
        y_send(q).start()

    @pl.loop(0, THIRD)
    def _(q):
        o_send(q).start()

    @pl.when(diag)
    def _():
        @pl.when(z < N - 1)
        def _():
            x_up(xt_ref, 0).start()

        @pl.when(z > 0)
        def _():
            x_dn(xt_ref, 0).start()

        cp = pltpu.make_async_copy(xr.at[:, pl.ds(0, rows)], xg_ref.at[0], aux.at[1])
        cp.start()
        cp.wait()

    w_load.wait()

    dist = jnp.abs(z - r)
    lag = jnp.where(z > r, N - 1 - z, jnp.where(z < r, z, jnp.maximum(z, N - 1 - z)))

    def x_step(c):
        for m in range(N):
            pos = jnp.where(dist == 0, (-1, 3, 6, 7)[m], 3 * (m + dist) - 1)

            @pl.when(c == pos)
            def _():
                x_send_like = far(xt_ref, xg_ref.at[m], x_s.at[0], x_r.at[m], r=z)
                x_send_like.wait_recv()

                @pl.when(has_up)
                def _():
                    x_up(xg_ref.at[m], m).start()

                @pl.when(has_dn)
                def _():
                    x_dn(xg_ref.at[m], m).start()

    def f_step(q):
        y_send(q).wait_recv()
        f_send(q).start()

    def load_pair(i):
        return pltpu.make_async_copy(dy_ref.at[piece(4 * i, 4)], dyv, ld.at[0])

    def load_other(i):
        return pltpu.make_async_copy(dyg_ref.at[0, piece(4 * i, 4)], dyv, ld.at[0])

    def load_far(q, size):
        return [pltpu.make_async_copy(dyg_ref.at[1 + h, where_rows(q)], dyv.at[pl.ds(h * size, size)], ld.at[h])
                for h in (0, 1)]

    def product(dsts, size):
        t = lax.dot_general(dyv[:len(dsts) * size], wv[...], (((1,), (1,)), ((), ())),
                            preferred_element_type=jnp.float32)
        for j, d in enumerate(dsts):
            d[...] = t[j * size:(j + 1) * size]

    def rows_of(ref, c):
        if isinstance(c, int) and c >= LAST:
            return ref.at[LAST, pl.ds((c - LAST) * p, p)]
        return ref.at[c]

    def by_size(c, fn):
        @pl.when(c < LAST)
        def _():
            fn(c)

        for j in (LAST, LAST + 1):
            @pl.when(c == j)
            def _():
                fn(j)

    def c_dn(c):
        return far(rows_of(pv, c), rows_of(upv, c), c_s.at[c], cu_r.at[c], c=z - 1)

    def c_up(c):
        return far(rows_of(pv, c), rows_of(dnv, c), c_s.at[c], cd_r.at[c], c=z + 1)

    def back(c, h, q, peer, off, size):
        return far(ov.at[min(c, LAST) if isinstance(c, int) else c, pl.ds(off, size)], dx_ref.at[where_rows(q)],
                   b_s.at[c, h], b_r.at[q], r=peer)

    def own_out(c):
        return pltpu.make_async_copy(ov.at[c], dx_ref.at[piece(2 * c, 2)], b_s.at[c, 0])

    def finish(c, start):
        def go(cp):
            if start:
                cp.start()
            else:
                cp.wait_send()

        if isinstance(c, int):
            q, off, h = c - PIECES, (c - LAST) * p, p // 2
            go(back(c, 0, q, r2, off, h))
            go(back(c, 1, q, r3, off + h, h))
            return

        @pl.when(c < THIRD)
        def _():
            if start:
                own_out(c).start()
            else:
                own_out(c).wait()

        @pl.when(jnp.logical_and(c >= THIRD, c < PIECES - 1))
        def _():
            go(back(c, 0, 2 * (c - THIRD), r1, 0, p))
            go(back(c, 1, 2 * (c - THIRD) + 1, r1, p, p))

        @pl.when(c == PIECES - 1)
        def _():
            go(back(PIECES - 1, 0, PIECES - 2, r1, 0, p))
            go(back(PIECES - 1, 1, PIECES - 1, r1, p, p // 2))
            go(back(PIECES - 1, 2, PIECES, r1, p + p // 2, p // 2))

        @pl.when(c >= PIECES)
        def _():
            go(back(c, 0, c - PIECES, r2, 0, p))
            go(back(c, 1, c - PIECES, r3, p, p))

    def sum_one(c):
        mine = rows_of(pv, c)

        @pl.when(has_up)
        def _():
            c_dn(c).wait_recv()
            mine[...] += rows_of(upv, c)[...]

        @pl.when(has_dn)
        def _():
            c_up(c).wait_recv()
            mine[...] += rows_of(dnv, c)[...]

        @pl.when(z > r)
        def _():
            c_dn(c).start()

        @pl.when(z < r)
        def _():
            c_up(c).start()

        @pl.when(diag)
        def _():
            rows_of(ov, c)[...] = mine[...].astype(jnp.bfloat16)
            finish(c, True)

    def sum_step(c):
        by_size(c, sum_one)

    ub = n // UNITS
    spans = ((0, rows), (rows, rows))

    def xr_load(m):
        o, cnt = spans[m]
        return pltpu.make_async_copy(xg_ref.at[m, :, pl.ds(0, cnt)], xr.at[:, pl.ds(o, cnt)], v_s.at[m])

    def unit_load(u, m):
        o, cnt = spans[m]
        cols = pl.ds(pl.multiple_of(u * ub, ub), ub)
        src = dy_ref.at[:, cols] if m == 0 else dyg_ref.at[m - 1, :, cols]
        return pltpu.make_async_copy(src, db.at[u % 2, pl.ds(o, cnt)], u_s.at[u % 2, m])

    def unit_out(u):
        cols = pl.ds(pl.multiple_of(u * ub, ub), ub)
        return pltpu.make_async_copy(ob.at[u % 2], dwp_ref.at[:, cols], u_s.at[u % 2, 2])

    def unit(u):
        @pl.when(u == 0)
        def _():
            for m in range(2):
                xr_load(m).start()
                unit_load(0, m).start()
            for m in range(2):
                xr_load(m).wait()

        @pl.when(u + 1 < UNITS)
        def _():
            for m in range(2):
                unit_load(u + 1, m).start()

        for m in range(2):
            unit_load(u, m).wait()

        @pl.when(u >= 2)
        def _():
            unit_out(u - 2).wait()

        ob[u % 2] = jnp.dot(xr[...], db[u % 2], preferred_element_type=jnp.float32)
        unit_out(u).start()

    end_lag = jnp.where(diag, jnp.minimum(lag, 1), 0)
    gap = lag - end_lag
    mid_lag = jnp.where(gap >= 1, lag - 1, lag)

    def after(c):
        now = jnp.where(c >= LAST - 2, jnp.where(c == LAST - 2, mid_lag, end_lag), lag)

        @pl.when(c >= now)
        def _():
            sum_step(c - now)

        @pl.when(jnp.logical_or(jnp.logical_and(c == LAST - 3, gap >= 1), jnp.logical_and(c == LAST - 2, gap >= 2)))
        def _():
            sum_one(c + 1 - now)

    base = jnp.where(r // 2 == z // 2, 6, 3)
    ahead = PIECES - base

    def f_early(c):
        @pl.when(jnp.logical_and(c >= base, (c - base) % 2 == 0))
        def _():
            q = (c - base) // 2

            @pl.when(q <= ahead)
            def _():
                f_step(q)

    u0 = jnp.where(dist == 0, 4, 3 * (1 + dist))

    def units(c):
        @pl.when(c >= u0)
        def _():
            @pl.loop(0, PER)
            def _(i):
                u = (c - u0) * PER + i

                @pl.when(u < UNITS)
                def _():
                    unit(u)

    load_pair(0).start()

    @pl.loop(0, THIRD)
    def _(i):
        c = 2 * i
        f_early(c)
        load_pair(0).wait()
        product([pv.at[c], pv.at[c + 1]], 2 * p)

        @pl.when(i + 1 < THIRD // 2)
        def _():
            load_pair(i + 1).start()

        @pl.when(jnp.logical_and(i + 1 >= THIRD // 2, i + 1 < THIRD))
        def _():
            k = i + 1 - THIRD // 2

            @pl.when(k == 0)
            def _():
                @pl.loop(0, THIRD)
                def _(q):
                    o_send(q).wait_recv()

            load_other(k).start()

        x_step(c)
        after(c)
        units(c)
        f_early(c + 1)
        x_step(c + 1)
        after(c + 1)
        units(c + 1)

    @pl.loop(PIECES, LAST)
    def _(c):
        q = c - PIECES
        f_early(c)

        @pl.when(q > ahead)
        def _():
            f_step(q)

        f_send(q).wait_recv()
        for cp in load_far(q, p):
            cp.start()
        for cp in load_far(q, p):
            cp.wait()
        product([pv.at[c]], 2 * p)
        x_step(c)
        after(c)
        units(c)

    for c in (LAST, LAST + 1):
        q = c - PIECES
        f_step(q)
        near, other = load_far(q, p // 2)
        near.start()
        f_send(q).wait_recv()
        other.start()
        near.wait()
        other.wait()
        product([rows_of(pv, c)], p)
        sum_step(c - end_lag)

    @pl.when(end_lag == 1)
    def _():
        sum_one(LAST + 1)

    for u in (UNITS - 2, UNITS - 1):
        unit_out(u).wait()

    @pl.when(jnp.logical_not(diag))
    def _():
        x_send().wait_send()

        @pl.loop(0, LAST)
        def _(c):
            c_dn(c).wait_send()

        for c in (LAST, LAST + 1):
            c_dn(c).wait_send()

        @pl.loop(0, PIECES - 1)
        def _(q):
            back(0, 0, q, r1, 0, p).wait_recv()

        for q in (PIECES - 1, PIECES):
            back(0, 0, q, r1, 0, p // 2).wait_recv()

    @pl.when(diag)
    def _():
        @pl.loop(0, LAST)
        def _(c):
            finish(c, False)

        for c in (LAST, LAST + 1):
            finish(c, False)

    for m in range(N):
        @pl.when(has_up)
        def _():
            x_up(xg_ref.at[m], m).wait_send()

        @pl.when(has_dn)
        def _():
            x_dn(xg_ref.at[m], m).wait_send()

    @pl.loop(0, PIECES - 1)
    def _(q):
        y_send(q).wait_send()
        f_send(q).wait_send()

    for q in (PIECES - 1, PIECES):
        y_send(q).wait_send()
        f_send(q).wait_send()

    @pl.loop(0, THIRD)
    def _(q):
        o_send(q).wait_send()


BLOCKS = 14
SLOTS = 6


def finish_grads(xg_ref, dyg_ref, dwp_ref, dxp_ref, dw_ref, dx_ref, xr, db, ob, dv, x_s, l_s, o_s, d_s):
    rows = dyg_ref.shape[1]
    bn = dw_ref.shape[1] // BLOCKS
    ahead = SLOTS - 2

    def load(u, h):
        cols, s = pl.ds(pl.multiple_of(u * bn, bn), bn), lax.rem(u, SLOTS)
        if h == 2:
            return pltpu.make_async_copy(dwp_ref.at[:, cols], ob.at[s], l_s.at[s, 2])
        return pltpu.make_async_copy(dyg_ref.at[1 + h, :, cols], db.at[s, pl.ds(h * rows, rows)], l_s.at[s, h])

    def out(u):
        cols, s = pl.ds(pl.multiple_of(u * bn, bn), bn), lax.rem(u, SLOTS)
        return pltpu.make_async_copy(ob.at[s], dw_ref.at[:, cols], o_s.at[s])

    xs = [pltpu.make_async_copy(xg_ref.at[2 + h], xr.at[:, pl.ds(h * rows, rows)], x_s.at[h])
          for h in (0, 1)]
    d_in = pltpu.make_async_copy(dxp_ref, dv, d_s.at[0])
    d_out = pltpu.make_async_copy(dv, dx_ref, d_s.at[1])
    for cp in xs:
        cp.start()

    @pl.loop(0, ahead)
    def _(u):
        for h in range(3):
            load(u, h).start()

    d_in.start()
    for cp in xs:
        cp.wait()

    @pl.loop(0, BLOCKS)
    def _(u):
        @pl.when(u >= 2)
        def _():
            out(u - 2).wait()

        @pl.when(u + ahead < BLOCKS)
        def _():
            for h in range(3):
                load(u + ahead, h).start()

        for h in range(3):
            load(u, h).wait()
        s = lax.rem(u, SLOTS)
        ob[s] += jnp.dot(xr[...], db[s], preferred_element_type=jnp.float32)
        out(u).start()

        @pl.when(u == 2)
        def _():
            d_in.wait()
            d_out.start()

    out(BLOCKS - 2).wait()
    out(BLOCKS - 1).wait()
    d_out.wait()


def solution(mesh):
    def local(x, w, dy):
        rows, n = dy.shape
        k = w.shape[0]
        p = rows // PIECES
        dma = pltpu.SemaphoreType.DMA
        bf, f32 = jnp.bfloat16, jnp.float32
        dx, dyg, xg, dwp, _ = pl.pallas_call(
            exchange,
            in_specs=[ANY] * 3,
            out_specs=[ANY] * 5,
            out_shape=[jax.ShapeDtypeStruct((rows, k), bf),
                       jax.ShapeDtypeStruct((N - 1, rows, n), bf),
                       jax.ShapeDtypeStruct((N, k, rows), bf),
                       jax.ShapeDtypeStruct((k, n), f32),
                       jax.ShapeDtypeStruct((k, rows), bf)],
            scratch_shapes=[
                pltpu.VMEM((k, n), bf), pltpu.VMEM((4 * p, n), bf),
                pltpu.VMEM((CHUNKS, 2 * p, k), f32), pltpu.VMEM((CHUNKS, 2 * p, k), f32),
                pltpu.VMEM((CHUNKS, 2 * p, k), f32), pltpu.VMEM((CHUNKS, 2 * p, k), bf),
                pltpu.VMEM((k, 2 * rows), bf),
                pltpu.VMEM((2, 2 * rows, n // UNITS), bf), pltpu.VMEM((2, k, n // UNITS), f32),
                dma((1,)), dma((N,)), dma((N,)), dma((N,)),
                dma((PARTS,)), dma((PARTS,)), dma((THIRD,)), dma((THIRD,)), dma((PARTS,)), dma((PARTS,)),
                dma((CHUNKS + 1,)), dma((CHUNKS + 1,)), dma((CHUNKS + 1,)), dma((CHUNKS + 1, 3)), dma((PARTS,)),
                dma((2,)), dma((2, 3)), dma((2,)), dma((2,)),
            ],
            compiler_params=pltpu.CompilerParams(collective_id=0, has_side_effects=True, vmem_limit_bytes=67043328),
            cost_estimate=pl.CostEstimate(flops=8 * rows * k * n, bytes_accessed=16 * rows * n, transcendentals=0),
            name="exchange",
        )(x.reshape(rows // (2 * p), 2 * p, k), w, dy)
        dw, dx = pl.pallas_call(
            finish_grads,
            in_specs=[ANY] * 4,
            out_specs=[ANY] * 2,
            out_shape=[jax.ShapeDtypeStruct((k, n), f32), jax.ShapeDtypeStruct((rows, k), bf)],
            scratch_shapes=[pltpu.VMEM((k, 2 * rows), bf), pltpu.VMEM((SLOTS, 2 * rows, n // BLOCKS), bf),
                            pltpu.VMEM((SLOTS, k, n // BLOCKS), f32), pltpu.VMEM((rows, k), bf),
                            dma((2,)), dma((SLOTS, 3)), dma((SLOTS,)), dma((2,))],
            compiler_params=pltpu.CompilerParams(vmem_limit_bytes=67043328),
            cost_estimate=pl.CostEstimate(flops=4 * rows * k * n, bytes_accessed=4 * rows * n + 8 * k * n,
                                          transcendentals=0),
            name="finish_grads",
        )(xg, dyg, dwp, dx)
        return dx, dw

    act = P(("dp", "r"), "c")
    return jax.shard_map(local, mesh=mesh, in_specs=(act, P("r", "c"), act),
                         out_specs=(act, act), check_vma=False)
```
